512 devices in a mesh: fsdp: 32 (over y, x, core), seq: 16 (over z).
Axes of the slice: x: 4, y: 4, z: 16, core: 2. Of those that a mesh axis runs over, the one named last changes fastest.
Arguments:
- query_rows: bfloat16 [64, 3072, 16, 128], P('fsdp', 'seq'), may hold values from -6 to 6
- key_rows: bfloat16 [64, 3072, 16, 128], P('fsdp', 'seq'), may hold values from -6 to 6
- value_rows: bfloat16 [64, 3072, 16, 128], P('fsdp', 'seq'), may hold values from -6 to 6
- gate_rows: bfloat16 [64, 3072, 16, 128], P('fsdp', 'seq'), may hold values from -6 to 6
- out_weight: bfloat16 [2048, 2048], P('fsdp'), may hold values from -0.125 to 0.125
Outputs:
- block_out: bfloat16 [64, 3072, 2048], P('fsdp', 'seq')
The draws below stay inside these ranges and needn't reach their ends.
All inputs are finite; a program needn't handle non-finite values.
Results may differ from the reference program's by a relative error of at most 0.006.
Values may be sent and summed in bfloat16 or wider, within the bound.
A program may use at most 64 MiB of HBM per device.

```python
import jax
import jax.numpy as jnp
from jax import lax

HEADS = 16
HEAD_SIZE = 128
BATCH = 64
TOKENS = 3072
WIDTH = 2048


def block_scale(own_key, dims, shards, low, top_value):
    loudness, own = 1.0, jax.random.fold_in(own_key, 6)
    for axis_at, blocks in shards:
        steps = jnp.exp(jax.random.uniform(jax.random.fold_in(own, axis_at), (blocks,), jnp.float32, low / len(shards), top_value / len(shards)))
        loudness = loudness * jnp.repeat(steps, dims[axis_at] // blocks).reshape([-1 if axis == axis_at else 1 for axis in range(len(dims))])
    return loudness


def gaussian(rng, extent, deviation, reach, split=(), dtype=jnp.bfloat16):
    drawn = jax.random.normal(rng, extent, jnp.float32) * deviation
    if len(split) > 0:
        drawn = block_scale(rng, extent, split, -0.22, 0.18) * drawn
    return jnp.clip(drawn, min=-reach, max=reach).astype(dtype)


def setup_inputs(seed: int = 0) -> dict:
    keys = jax.random.split(jax.random.key(seed), 6)
    query_rows = gaussian(keys[0], (BATCH, TOKENS, HEADS, HEAD_SIZE), 1.0, 6.0, ((0, 32), (1, 16)))
    key_rows = gaussian(keys[1], (BATCH, TOKENS, HEADS, HEAD_SIZE), 1.0, 6.0, ((0, 32), (1, 16)))
    value_rows = gaussian(keys[2], (BATCH, TOKENS, HEADS, HEAD_SIZE), 1.0, 6.0, ((0, 32), (1, 16)))
    gate_rows = gaussian(keys[3], (BATCH, TOKENS, HEADS, HEAD_SIZE), 1.0, 6.0, ((0, 32), (1, 16)))
    out_weight = gaussian(keys[4], (WIDTH, WIDTH), WIDTH ** -0.5, 0.125, ((0, 32),))
    return dict(query_rows=query_rows, key_rows=key_rows, value_rows=value_rows, gate_rows=gate_rows, out_weight=out_weight)


def feature_map(values):
    wide = values.astype(jnp.float32)
    return (wide * wide + 0.1).astype(jnp.bfloat16)


def finish_heads(read, gate_rows, count):
    result = read * count ** 0.5
    result = result * jax.nn.sigmoid(gate_rows.astype(jnp.float32))
    return result.astype(jnp.bfloat16)


def read_state(features, state, mass):
    small = lax.optimization_barrier(state.astype(jnp.bfloat16))
    top = jnp.einsum("bthd,bhde->bthe", features.astype(jnp.float32), small.astype(jnp.float32))
    bottom = jnp.einsum("bthd,bhd->bth", features.astype(jnp.float32), mass, precision=lax.Precision.HIGHEST)
    return top / (bottom + 1e-3)[..., None]


def reference(query_rows, key_rows, value_rows, gate_rows, out_weight):
    query_feature, key_feature = lax.optimization_barrier((feature_map(query_rows), feature_map(key_rows)))
    state = jnp.einsum("bthd,bthe->bhde", key_feature.astype(jnp.float32), value_rows.astype(jnp.float32)) / TOKENS
    mass = jnp.sum(key_feature.astype(jnp.float32), axis=1) / TOKENS
    mixed = finish_heads(read_state(query_feature, state, mass), gate_rows, TOKENS).reshape(BATCH, TOKENS, WIDTH)
    mixed = lax.optimization_barrier(mixed)
    block_out = jnp.einsum("btw,wv->btv", mixed.astype(jnp.float32), out_weight.astype(jnp.float32)).astype(jnp.bfloat16)
    return block_out
```

```python
import functools

import jax
import jax.numpy as jnp
from jax import lax
from jax.experimental import pallas as pl
from jax.experimental.pallas import tpu as pltpu
from jax.sharding import PartitionSpec as P

MESH = pl.DeviceIdType.MESH
F32, BF16 = jnp.float32, jnp.bfloat16
BLOCK = 32
UP, DOWN = 0, 1


def feature(raw):
    wide = raw.astype(F32)
    return wide * wide + 0.1


def layer_kernel(
    ny, nx, nz, count,
    q_hbm, k_hbm, v_hbm, g_hbm, w_hbm, out_ref,
    q_raw, k_raw, v_raw, g_raw, q_feat, k_feat, v_head, gates,
    part, other, sums, states, weight, mixed, total,
    load_sem, part_send, part_recv, rs_send, rs_recv, ag_send, ag_recv,
    hand_send, hand_recv, line_send, line_recv, push_send, push_recv, own_send, own_recv,
):
    seqs, tokens, heads, size = k_raw.shape
    width = weight.shape[2]
    half = weight.shape[1] // 2
    state_rows = 2 * seqs * size
    z, f = lax.axis_index("seq"), lax.axis_index("fsdp")
    core = lax.rem(f, 2)
    chip = f // 2
    x, y = lax.rem(chip, nx), chip // nx
    above, below = lax.rem(z + 1, nz), lax.rem(z + nz - 1, nz)
    partner = {"fsdp": chip * 2 + 1 - core}
    barrier = pltpu.get_barrier_semaphore()

    def head_at(offset):
        return lax.rem(z + offset + 2 * nz, nz)

    loads = [
        pltpu.make_async_copy(src, dst, load_sem.at[at])
        for at, (src, dst) in enumerate(((k_hbm, k_raw), (v_hbm, v_raw), (q_hbm, q_raw), (g_hbm, g_raw)))
    ]
    own_rows = weight.at[chip, pl.ds(pl.multiple_of(core * half, half), half)]
    loads.append(pltpu.make_async_copy(w_hbm, own_rows, load_sem.at[4]))

    def by_head(values):
        return jnp.swapaxes(values, 0, 1)

    def relayout(s, t):
        rows = pl.ds(pl.multiple_of(t, BLOCK), BLOCK)
        k_feat[:, s, rows, :] = by_head(feature(k_raw[s, rows])).astype(BF16)
        v_head[:, s, rows, :] = by_head(v_raw[s, rows].astype(F32)).astype(BF16)

    def relayout_all():
        for s in range(seqs):
            @pl.loop(0, tokens // BLOCK)
            def _(i):
                relayout(s, i * BLOCK)

    def relayout_late(unit):
        per_seq = tokens // BLOCK
        s = unit // per_seq
        rows = pl.ds(pl.multiple_of(lax.rem(unit, per_seq) * BLOCK, BLOCK), BLOCK)
        q_feat[:, s, rows, :] = by_head(feature(q_raw[s, rows])).astype(BF16)
        gate = g_raw[s, rows].astype(F32)
        gates[:, s, rows, :] = by_head(count**0.5 / (1.0 + jnp.exp(-gate)))

    late_units = seqs * tokens // BLOCK

    def partial(head, first_row):
        ones = jnp.ones((8, tokens), BF16)
        place = lax.broadcasted_iota(jnp.int32, (8, size), 0)
        mass = jnp.zeros((8, size), F32)
        for s in range(seqs):
            keys = k_feat[head, s]
            part[head, s * size:(s + 1) * size, :] = lax.dot_general(
                keys, v_head[head, s], (((0,), (0,)), ((), ())), preferred_element_type=F32
            )
            row = jnp.dot(ones, keys, preferred_element_type=F32)
            mass = jnp.where(place == first_row + s, row, mass)
        part[head, seqs * size:, :] = mass

    def read_head(head, first_row):
        tail = states[head, state_rows:, :].astype(F32)
        for s in range(seqs):
            row = first_row + s
            feats = q_feat[head, s]
            top = jnp.dot(
                feats, states[head, row * size:(row + 1) * size, :], preferred_element_type=F32
            )
            mass = tail[row:row + 1] + tail[8 + row:9 + row]
            bottom = jnp.sum(feats.astype(F32) * mass, axis=1, keepdims=True)
            read = top * (1.0 / (bottom + 0.001))
            mixed[head, s * tokens:(s + 1) * tokens, :] = (read * gates[head, s]).astype(BF16)

    def project(a, b, first=False, last=False):
        rows = jnp.concatenate([mixed[a], mixed[b]], axis=1)
        step = 512

        @pl.loop(0, width // step)
        def _(i):
            cols = pl.ds(pl.multiple_of(i * step, step), step)
            piece = jnp.dot(
                rows, jnp.concatenate([weight[a, :, cols], weight[b, :, cols]], axis=0),
                preferred_element_type=F32,
            )
            if not first:
                piece = total[:, cols] + piece
            if last:
                for s in range(seqs):
                    out_ref[s, :, cols] = piece[s * tokens:(s + 1) * tokens].astype(BF16)
            else:
                total[:, cols] = piece

    def part_copy(head):
        return pltpu.make_async_remote_copy(
            part.at[head], other.at[head], part_send.at[head], part_recv.at[head],
            device_id=partner, device_id_type=MESH,
        )

    def hand_copy(head):
        rows = pl.ds(seqs * size, state_rows + 16 - seqs * size)
        return pltpu.make_async_remote_copy(
            states.at[head, rows], states.at[head, rows], hand_send.at[head], hand_recv.at[head],
            device_id=partner, device_id_type=MESH,
        )

    def push_copy(piece, which):
        rows = pl.ds(which * half, half)
        return pltpu.make_async_remote_copy(
            weight.at[piece, rows], weight.at[piece, rows],
            push_send.at[piece, which], push_recv.at[piece, which],
            device_id=partner, device_id_type=MESH,
        )

    def own_copy():
        return pltpu.make_async_remote_copy(
            w_hbm, weight.at[chip, pl.ds(half, half)], own_send, own_recv,
            device_id=partner, device_id_type=MESH,
        )

    @pl.when(core == 1)
    def _ring():
        for load in loads:
            load.start()
        for device in ({"seq": above}, {"seq": below}, partner):
            pl.semaphore_signal(barrier, inc=1, device_id=device, device_id_type=MESH)
        loads[0].wait()
        loads[1].wait()
        relayout_all()
        partial(head_at(nz // 2), 0)
        pl.semaphore_wait(barrier, 3)
        own_copy().start()

        pieces = 2 * seqs
        spans = [(i * size, size if i < pieces - 1 else size + 16) for i in range(pieces)]
        early = jnp.where(lax.rem(z, 4) < 2, DOWN, UP)

        def target(d):
            return {"seq": jnp.where(d == UP, above, below)}

        def rs_copy(k, d, i):
            rows = pl.ds(*spans[i])
            return pltpu.make_async_remote_copy(
                sums.at[d, k, rows], sums.at[d, k + 1, rows], rs_send.at[k, d, i], rs_recv.at[k, d, i],
                device_id=target(d), device_id_type=MESH,
            )

        def ag_copy(k, d, i):
            rows = pl.ds(*spans[i])
            head = head_at(jnp.where(d == UP, -k, k))
            return pltpu.make_async_remote_copy(
                states.at[head, rows], states.at[head, rows], ag_send.at[k, d, i], ag_recv.at[k, d, i],
                device_id=target(d), device_id_type=MESH,
            )

        def ag_arrived(k, d, i):
            rows = pl.ds(*spans[i])
            head = head_at(jnp.where(d == UP, -k - 1, k + 1))
            pltpu.make_async_remote_copy(
                states.at[head, rows], states.at[head, rows], ag_send.at[k, d, i], ag_recv.at[k, d, i],
                device_id=target(d), device_id_type=MESH,
            ).wait_recv()

        def own_sum(head, i):
            if i < seqs:
                return part[head, i * size:(i + 1) * size, :]
            return other[head, (i - seqs) * size:(i - seqs + 1) * size, :]

        def own_mass(head):
            return part[head, seqs * size:, :] + other[head, seqs * size:, :]

        def split(mass):
            high = mass.astype(BF16)
            return jnp.concatenate([high.astype(F32), mass - high.astype(F32)], axis=0).astype(BF16)

        def add_and_send(k, d, i, received):
            head = head_at(jnp.where(d == UP, nz // 2 - k, nz // 2 + k))
            start = i * size
            value = own_sum(head, i)
            if received:
                rs_copy(k - 1, d, i).wait_recv()
                value = value + sums[d, k, start:start + size, :].astype(F32)
            sums[d, k, start:start + size, :] = value.astype(BF16)
            if i == pieces - 1:
                mass = own_mass(head)
                if received:
                    old = sums[d, k, state_rows:, :].astype(F32)
                    mass = mass + old[:8] + old[8:]
                sums[d, k, state_rows:, :] = split(mass)
            rs_copy(k, d, i).start()

        def first_way(i):
            return DOWN if i < seqs else UP

        for i in range(pieces):
            if i == seqs:
                part_copy(head_at(nz // 2)).wait_recv()
            add_and_send(0, first_way(i), i, False)
        partial(head_at(nz // 2 + 1), 0)
        partial(head_at(nz // 2 - 1), 0)
        for i in range(pieces):
            if i == seqs:
                part_copy(head_at(nz // 2 + 1)).wait_recv()
                part_copy(head_at(nz // 2 - 1)).wait_recv()
            add_and_send(1, 1 - first_way(i), i, False)
            add_and_send(1, first_way(i), i, True)
        partial(head_at(nz // 2 + 2), 0)
        partial(head_at(nz // 2 - 2), 0)
        loads[2].wait()
        loads[3].wait()

        per_step = -(-late_units // (nz // 2 - 2))

        @pl.loop(2, nz // 2)
        def _(k):
            for i in range(pieces):
                if i == seqs:
                    part_copy(head_at(nz // 2 + k)).wait_recv()
                    part_copy(head_at(nz // 2 - k)).wait_recv()
                add_and_send(k, early, i, True)
                add_and_send(k, 1 - early, i, True)

            @pl.when(k < nz // 2 - 1)
            def _():
                partial(head_at(nz // 2 + k + 1), 0)
                partial(head_at(nz // 2 - k - 1), 0)

            @pl.when(k == nz // 2 - 1)
            def _():
                partial(head_at(0), 0)

            for j in range(per_step):
                relayout_late((k - 2) * per_step + j)

        order = list(range(seqs, pieces)) + list(range(seqs))
        part_copy(z).wait_recv()
        for i in order:
            start = i * size
            value = own_sum(z, i)
            for d in (DOWN, UP):
                rs_copy(nz // 2 - 1, d, i).wait_recv()
                value = value + sums[d, nz // 2, start:start + size, :].astype(F32)
            states[z, start:start + size, :] = (value * (1.0 / count)).astype(BF16)
            if i == pieces - 1:
                mass = own_mass(z)
                for d in (DOWN, UP):
                    old = sums[d, nz // 2, state_rows:, :].astype(F32)
                    mass = mass + old[:8] + old[8:]
                states[z, state_rows:, :] = split(mass * (1.0 / count))
            ag_copy(0, UP, i).start()
            ag_copy(0, DOWN, i).start()
            if i == pieces - 1:
                hand_copy(z).start()

        def pass_on(k, both):
            for i in order:
                if both:
                    for d in (early, 1 - early):
                        ag_arrived(k - 1, d, i)
                        ag_copy(k, d, i).start()
                else:
                    for d in (UP, DOWN):
                        ag_arrived(k - 1, d, i)
                    ag_copy(k, 1 - first_way(i), i).start()
                if i == pieces - 1:
                    hand_copy(head_at(-k)).start()
                    hand_copy(head_at(k)).start()

        def weights_here():
            for offset in range(nx * ny):
                piece = lax.rem(chip + offset, nx * ny)
                push_copy(piece, 0).wait_recv()
                if offset > 0:
                    push_copy(piece, 1).wait_recv()

        def read_pair(k):
            read_head(head_at(-k), 0)
            read_head(head_at(k), 0)

        pass_on(1, True)
        read_head(z, 0)
        read_pair(1)
        pass_on(2, True)
        read_pair(2)
        loads[4].wait()
        weights_here()
        project(head_at(-1), head_at(1), first=True)

        @pl.loop(3, nz // 2 - 1)
        def _(k):
            pass_on(k, True)
            read_pair(k)
            project(head_at(1 - k), head_at(k - 1))

        pass_on(nz // 2 - 1, False)
        read_pair(nz // 2 - 1)
        project(head_at(2 - nz // 2), head_at(nz // 2 - 2))
        for i in order:
            ag_arrived(nz // 2 - 1, 1 - first_way(i), i)
            if i == pieces - 1:
                hand_copy(head_at(nz // 2)).start()
        project(head_at(1 - nz // 2), head_at(nz // 2 - 1))
        read_head(head_at(nz // 2), 0)
        project(z, head_at(nz // 2), last=True)

        own_copy().wait_send()
        for i in range(pieces):
            rs_copy(0, first_way(i), i).wait_send()
            ag_copy(nz // 2 - 1, 1 - first_way(i), i).wait_send()

        @pl.loop(0, nz // 2 - 1)
        def _(k):
            for i in range(pieces):
                for d in (UP, DOWN):
                    rs_copy(k + 1, d, i).wait_send()
                    ag_copy(k, d, i).wait_send()

        @pl.loop(0, nz)
        def _(j):
            hand_copy(j).wait_send()

    @pl.when(core == 0)
    def _weights():
        for load in loads:
            load.start()
        east, west = y * nx + lax.rem(x + 1, nx), y * nx + lax.rem(x + nx - 1, nx)
        north, south = lax.rem(y + 1, ny) * nx + x, lax.rem(y + ny - 1, ny) * nx + x
        ways = ((east, west), (north, south))
        for device in (east, west, north, south):
            pl.semaphore_signal(barrier, inc=1, device_id={"fsdp": device * 2}, device_id_type=MESH)
        pl.semaphore_signal(barrier, inc=1, device_id=partner, device_id_type=MESH)

        items = (((0, 0), (1, 0), (1, -1), (1, 1), (1, 2)), ((1, 0), (0, 0), (0, -1), (0, 1), (0, 2)))

        def piece_at(axis, item, along):
            across = items[axis][item][1]
            dx, dy = (along, across) if axis == 0 else (across, along)
            return lax.rem(y + dy + ny, ny) * nx + lax.rem(x + dx + nx, nx)

        def line_copy(axis, item, way, stage, arriving):
            sign = 1 if way == 0 else -1
            if stage == 0:
                along, start, rows = 0, 0, half
            else:
                along, start, rows = -sign, way * (half // 2), half // 2
            if arriving:
                along = along - sign
                along = 2 if along == -2 else along
            spot = weight.at[piece_at(axis, item, along), pl.ds(items[axis][item][0] * half + start, rows)]
            return pltpu.make_async_remote_copy(
                spot, spot, line_send.at[axis, item, way, stage], line_recv.at[axis, item, way, stage],
                device_id={"fsdp": ways[axis][way] * 2}, device_id_type=MESH,
            )

        def send(axis, item):
            for way in (0, 1):
                line_copy(axis, item, way, 0, False).start()

        def got(axis, item, stage):
            for way in (0, 1):
                line_copy(axis, item, way, stage, True).wait_recv()

        def forward(axis, item):
            for way in (0, 1):
                line_copy(axis, item, way, 0, True).wait_recv()
                line_copy(axis, item, way, 1, False).start()

        def at(dx, dy):
            return lax.rem(y + dy + ny, ny) * nx + lax.rem(x + dx + nx, nx)

        def push(dx, dy, which):
            push_copy(at(dx, dy), which).start()

        loads[0].wait()
        loads[1].wait()
        relayout_all()
        pl.semaphore_wait(barrier, 5)
        loads[4].wait()
        send(0, 0)
        send(1, 1)

        def part_out(offset):
            partial(head_at(offset), seqs)
            part_copy(head_at(offset)).start()

        part_out(nz // 2)

        @pl.loop(1, nz // 2)
        def _(k):
            part_out(nz // 2 + k)
            part_out(nz // 2 - k)

            @pl.when(k == 2)
            def _():
                own_copy().wait_recv()
                send(1, 0)
                send(0, 1)

        part_out(0)
        push(0, 0, 0)
        loads[2].wait()
        loads[3].wait()

        @pl.loop(0, late_units // 2)
        def _(i):
            relayout_late(i)

        forward(0, 0)
        send(1, 2)
        send(1, 3)
        push(-1, 0, 0)
        push(1, 0, 0)
        forward(1, 0)
        send(0, 2)
        send(0, 3)
        push(0, -1, 1)
        push(0, 1, 1)

        @pl.loop(late_units // 2, late_units)
        def _(i):
            relayout_late(i)

        forward(0, 1)
        forward(1, 1)
        push(-1, 0, 1)
        push(1, 0, 1)
        push(0, -1, 0)
        push(0, 1, 0)
        got(0, 0, 1)
        send(1, 4)
        push(2, 0, 0)
        got(1, 0, 1)
        send(0, 4)
        push(0, 2, 1)
        for item, off in ((2, -1), (3, 1)):
            forward(1, item)
            push(off, -1, 0)
            push(off, 1, 0)
            forward(0, item)
            push(-1, off, 1)
            push(1, off, 1)
        got(0, 1, 1)
        push(2, 0, 1)
        got(1, 1, 1)
        push(0, 2, 0)
        forward(1, 4)
        push(2, -1, 0)
        push(2, 1, 0)
        forward(0, 4)
        push(-1, 2, 1)
        push(1, 2, 1)
        for item, off in ((2, -1), (3, 1), (4, 2)):
            got(1, item, 1)
            push(off, 2, 0)
            got(0, item, 1)
            push(2, off, 1)

        hand_copy(z).wait_recv()
        read_head(z, seqs)

        def read_pair(k):
            for head in (head_at(-k), head_at(k)):
                hand_copy(head).wait_recv()
                read_head(head, seqs)

        read_pair(1)
        project(head_at(-1), head_at(1), first=True)

        @pl.loop(2, nz // 2)
        def _(k):
            read_pair(k)
            project(head_at(-k), head_at(k))

        hand_copy(head_at(nz // 2)).wait_recv()
        read_head(head_at(nz // 2), seqs)
        project(z, head_at(nz // 2), last=True)

        for axis in (0, 1):
            for item in range(5):
                for way in (0, 1):
                    for stage in (0, 1):
                        line_copy(axis, item, way, stage, False).wait_send()

        @pl.loop(0, nz)
        def _(j):
            part_copy(j).wait_send()

        for offset in range(nx * ny):
            piece = lax.rem(chip + offset, nx * ny)
            push_copy(piece, 0).wait_send()
            if offset > 0:
                push_copy(piece, 1).wait_send()


def local(ny, nx, nz, query_rows, key_rows, value_rows, gate_rows, out_weight):
    seqs, tokens, heads, size = query_rows.shape
    rows, width = out_weight.shape
    chips = nx * ny
    raw = pltpu.VMEM((seqs, tokens, heads, size), BF16)
    split = pltpu.VMEM((heads, seqs, tokens, size), BF16)
    part = pltpu.VMEM((heads, seqs * size + 8, size), F32)
    chunk = 2 * seqs * size + 16
    dma = pltpu.SemaphoreType.DMA
    return pl.pallas_call(
        functools.partial(layer_kernel, ny, nx, nz, float(tokens * nz)),
        name="layer",
        out_shape=jax.ShapeDtypeStruct((seqs, tokens, width), BF16),
        in_specs=[pl.BlockSpec(memory_space=pl.ANY)] * 5,
        out_specs=pl.BlockSpec(memory_space=pltpu.VMEM),
        scratch_shapes=[
            raw, raw, raw, raw,
            split, split, split,
            pltpu.VMEM((heads, seqs, tokens, size), F32),
            part, part,
            pltpu.VMEM((2, nz // 2 + 1, chunk, size), BF16),
            pltpu.VMEM((heads, chunk, size), BF16),
            pltpu.VMEM((chips, 2 * rows, width), BF16),
            pltpu.VMEM((heads, seqs * tokens, size), BF16),
            pltpu.VMEM((seqs * tokens, width), F32),
            dma((5,)),
            dma((heads,)), dma((heads,)),
            dma((nz // 2, 2, 2 * seqs)), dma((nz // 2, 2, 2 * seqs)),
            dma((nz // 2, 2, 2 * seqs)), dma((nz // 2, 2, 2 * seqs)),
            dma((heads,)), dma((heads,)),
            dma((2, 5, 2, 2)), dma((2, 5, 2, 2)),
            dma((chips, 2)), dma((chips, 2)),
            dma, dma,
        ],
        compiler_params=pltpu.CompilerParams(
            collective_id=0, has_side_effects=True, vmem_limit_bytes=60 * 2**20
        ),
    )(query_rows, key_rows, value_rows, gate_rows, out_weight)


def solution(mesh):
    in_specs = (
        P("fsdp", "seq", None, None),
        P("fsdp", "seq", None, None),
        P("fsdp", "seq", None, None),
        P("fsdp", "seq", None, None),
        P("fsdp", None),
    )
    out_specs = P("fsdp", "seq", None)
    body = functools.partial(local, 4, 4, mesh.shape["seq"])
    return jax.shard_map(body, mesh=mesh, in_specs=in_specs, out_specs=out_specs, check_vma=False)
```

```python
import functools

import jax
import jax.numpy as jnp
from jax import lax
from jax.experimental import pallas as pl
from jax.experimental.pallas import tpu as pltpu
from jax.sharding import PartitionSpec as P

MESH = pl.DeviceIdType.MESH
F32, BF16 = jnp.float32, jnp.bfloat16
BLOCK = 32
UP, DOWN = 0, 1


def feature(raw):
    wide = raw.astype(F32)
    return wide * wide + 0.1


def layer_kernel(
    ny, nx, nz, count,
    q_hbm, k_hbm, v_hbm, g_hbm, w_hbm, out_ref,
    q_raw, k_raw, v_raw, g_raw, q_feat, k_feat, v_head, gates,
    part, other, sums, states, weight, mixed, total,
    load_sem, part_send, part_recv, rs_send, rs_recv, ag_send, ag_recv,
    hand_send, hand_recv, line_send, line_recv, push_send, push_recv, own_send, own_recv,
):
    seqs, tokens, heads, size = k_raw.shape
    width = weight.shape[2]
    half = weight.shape[1] // 2
    state_rows = 2 * seqs * size
    z, f = lax.axis_index("seq"), lax.axis_index("fsdp")
    core = lax.rem(f, 2)
    chip = f // 2
    x, y = lax.rem(chip, nx), chip // nx
    above, below = lax.rem(z + 1, nz), lax.rem(z + nz - 1, nz)
    partner = {"fsdp": chip * 2 + 1 - core}
    barrier = pltpu.get_barrier_semaphore()

    def head_at(offset):
        return lax.rem(z + offset + 2 * nz, nz)

    key_loads, value_loads = (
        [pltpu.make_async_copy(src.at[s], dst.at[s], load_sem.at[at, s]) for s in range(seqs)]
        for at, (src, dst) in enumerate(((k_hbm, k_raw), (v_hbm, v_raw)))
    )
    late_loads = [
        pltpu.make_async_copy(src, dst, load_sem.at[2, at])
        for at, (src, dst) in enumerate(((q_hbm, q_raw), (g_hbm, g_raw)))
    ]
    own_rows = weight.at[chip, pl.ds(pl.multiple_of(core * half, half), half)]
    own_load = pltpu.make_async_copy(w_hbm, own_rows, load_sem.at[3, 0])

    def start_loads():
        for s in range(seqs):
            key_loads[s].start()
            value_loads[s].start()
        own_load.start()
        for load in late_loads:
            load.start()

    def by_head(values):
        return jnp.swapaxes(values, 0, 1)

    group = heads // 2

    def relayout(which, wait):
        span = slice(which * group, (which + 1) * group)
        for s in range(seqs):
            for load, src, dst, fn in (
                (key_loads[s], k_raw, k_feat, feature),
                (value_loads[s], v_raw, v_head, lambda raw: raw.astype(F32)),
            ):
                if wait:
                    load.wait()

                @pl.loop(0, tokens // BLOCK)
                def _(i):
                    rows = pl.ds(pl.multiple_of(i * BLOCK, BLOCK), BLOCK)
                    dst[span, s, rows, :] = by_head(fn(src[s, rows, span])).astype(BF16)

    starts_late = z >= nz // 2

    def relayout_first():
        relayout(0, True)

        @pl.when(jnp.logical_not(starts_late))
        def _():
            relayout(1, False)

    def relayout_rest():
        @pl.when(starts_late)
        def _():
            relayout(1, False)

    def relayout_late(unit):
        per_seq = tokens // BLOCK
        s = unit // per_seq
        rows = pl.ds(pl.multiple_of(lax.rem(unit, per_seq) * BLOCK, BLOCK), BLOCK)
        q_feat[:, s, rows, :] = by_head(feature(q_raw[s, rows])).astype(BF16)
        gate = g_raw[s, rows].astype(F32)
        gates[:, s, rows, :] = by_head(count**0.5 / (1.0 + jnp.exp(-gate)))

    late_units = seqs * tokens // BLOCK

    def partial(head, first_row):
        ones = jnp.ones((8, tokens), BF16)
        place = lax.broadcasted_iota(jnp.int32, (8, size), 0)
        mass = jnp.zeros((8, size), F32)
        for s in range(seqs):
            keys = k_feat[head, s]
            part[head, s * size:(s + 1) * size, :] = lax.dot_general(
                keys, v_head[head, s], (((0,), (0,)), ((), ())), preferred_element_type=F32
            )
            row = jnp.dot(ones, keys, preferred_element_type=F32)
            mass = jnp.where(place == first_row + s, row, mass)
        part[head, seqs * size:, :] = mass

    def read_part(head, first_row, s):
        tail = states[head, state_rows:, :].astype(F32)
        row = first_row + s
        feats = q_feat[head, s]
        top = jnp.dot(feats, states[head, row * size:(row + 1) * size, :], preferred_element_type=F32)
        mass = tail[row:row + 1] + tail[8 + row:9 + row]
        bottom = jnp.sum(feats.astype(F32) * mass, axis=1, keepdims=True)
        read = top * (1.0 / (bottom + 0.001))
        mixed[head, s * tokens:(s + 1) * tokens, :] = (read * gates[head, s]).astype(BF16)

    def read_head(head, first_row):
        for s in range(seqs):
            read_part(head, first_row, s)

    step = width // 4

    def project_part(a, b, i, first=False, last=False):
        rows = jnp.concatenate([mixed[a], mixed[b]], axis=1)
        cols = pl.ds(pl.multiple_of(i * step, step), step)
        piece = jnp.dot(
            rows, jnp.concatenate([weight[a, :, cols], weight[b, :, cols]], axis=0),
            preferred_element_type=F32,
        )
        if not first:
            piece = total[:, cols] + piece
        if last:
            for s in range(seqs):
                out_ref[s, :, cols] = piece[s * tokens:(s + 1) * tokens].astype(BF16)
        else:
            total[:, cols] = piece

    def project(a, b, first=False, last=False):
        @pl.loop(0, width // step)
        def _(i):
            project_part(a, b, i, first, last)

    def part_copy(head):
        return pltpu.make_async_remote_copy(
            part.at[head], other.at[head], part_send.at[head], part_recv.at[head],
            device_id=partner, device_id_type=MESH,
        )

    def hand_copy(head):
        rows = pl.ds(seqs * size, state_rows + 16 - seqs * size)
        return pltpu.make_async_remote_copy(
            states.at[head, rows], states.at[head, rows], hand_send.at[head], hand_recv.at[head],
            device_id=partner, device_id_type=MESH,
        )

    def push_copy(piece, which):
        rows = pl.ds(which * half, half)
        return pltpu.make_async_remote_copy(
            weight.at[piece, rows], weight.at[piece, rows],
            push_send.at[piece, which], push_recv.at[piece, which],
            device_id=partner, device_id_type=MESH,
        )

    def own_copy():
        return pltpu.make_async_remote_copy(
            w_hbm, weight.at[chip, pl.ds(half, half)], own_send, own_recv,
            device_id=partner, device_id_type=MESH,
        )

    @pl.when(core == 1)
    def _ring():
        start_loads()
        for device in ({"seq": above}, {"seq": below}, partner):
            pl.semaphore_signal(barrier, inc=1, device_id=device, device_id_type=MESH)
        relayout_first()
        partial(head_at(nz // 2), 0)
        pl.semaphore_wait(barrier, 3)
        own_copy().start()

        pieces = 2 * seqs
        spans = [(i * size, size if i < pieces - 1 else size + 16) for i in range(pieces)]
        early = jnp.where(lax.rem(z, 4) < 2, DOWN, UP)

        def target(d):
            return {"seq": jnp.where(d == UP, above, below)}

        def rs_copy(k, d, i):
            rows = pl.ds(*spans[i])
            return pltpu.make_async_remote_copy(
                sums.at[d, k, rows], sums.at[d, k + 1, rows], rs_send.at[k, d, i], rs_recv.at[k, d, i],
                device_id=target(d), device_id_type=MESH,
            )

        def ag_copy(k, d, i):
            rows = pl.ds(*spans[i])
            head = head_at(jnp.where(d == UP, -k, k))
            return pltpu.make_async_remote_copy(
                states.at[head, rows], states.at[head, rows], ag_send.at[k, d, i], ag_recv.at[k, d, i],
                device_id=target(d), device_id_type=MESH,
            )

        def ag_arrived(k, d, i):
            rows = pl.ds(*spans[i])
            head = head_at(jnp.where(d == UP, -k - 1, k + 1))
            pltpu.make_async_remote_copy(
                states.at[head, rows], states.at[head, rows], ag_send.at[k, d, i], ag_recv.at[k, d, i],
                device_id=target(d), device_id_type=MESH,
            ).wait_recv()

        def own_sum(head, i):
            if i < seqs:
                return part[head, i * size:(i + 1) * size, :]
            return other[head, (i - seqs) * size:(i - seqs + 1) * size, :]

        def own_mass(head):
            return part[head, seqs * size:, :] + other[head, seqs * size:, :]

        def split(mass):
            high = mass.astype(BF16)
            return jnp.concatenate([high.astype(F32), mass - high.astype(F32)], axis=0).astype(BF16)

        def add_and_send(k, d, i, received):
            head = head_at(jnp.where(d == UP, nz // 2 - k, nz // 2 + k))
            start = i * size
            value = own_sum(head, i)
            if received:
                rs_copy(k - 1, d, i).wait_recv()
                value = value + sums[d, k, start:start + size, :].astype(F32)
            sums[d, k, start:start + size, :] = value.astype(BF16)
            if i == pieces - 1:
                mass = own_mass(head)
                if received:
                    old = sums[d, k, state_rows:, :].astype(F32)
                    mass = mass + old[:8] + old[8:]
                sums[d, k, state_rows:, :] = split(mass)
            rs_copy(k, d, i).start()

        def first_way(i):
            return DOWN if i < seqs else UP

        for i in range(pieces):
            if i == seqs:
                part_copy(head_at(nz // 2)).wait_recv()
            add_and_send(0, first_way(i), i, False)
        relayout_rest()
        partial(head_at(nz // 2 + 1), 0)
        partial(head_at(nz // 2 - 1), 0)
        for i in range(pieces):
            if i == seqs:
                part_copy(head_at(nz // 2 + 1)).wait_recv()
                part_copy(head_at(nz // 2 - 1)).wait_recv()
            add_and_send(1, 1 - first_way(i), i, False)
            add_and_send(1, first_way(i), i, True)
        partial(head_at(nz // 2 + 2), 0)
        partial(head_at(nz // 2 - 2), 0)
        for load in late_loads:
            load.wait()

        per_step = -(-late_units // (nz // 2 - 2))

        @pl.loop(2, nz // 2)
        def _(k):
            for i in range(pieces):
                if i == seqs:
                    part_copy(head_at(nz // 2 + k)).wait_recv()
                    part_copy(head_at(nz // 2 - k)).wait_recv()
                add_and_send(k, early, i, True)
                add_and_send(k, 1 - early, i, True)

            @pl.when(k < nz // 2 - 1)
            def _():
                partial(head_at(nz // 2 + k + 1), 0)
                partial(head_at(nz // 2 - k - 1), 0)

            @pl.when(k == nz // 2 - 1)
            def _():
                partial(head_at(0), 0)

            for j in range(per_step):
                relayout_late((k - 2) * per_step + j)
            rows = seqs * tokens // (nz // 2 - 2)
            total[pl.ds(pl.multiple_of((k - 2) * rows, 8), rows), :] = jnp.zeros((rows, width), F32)

        order = list(range(seqs, pieces)) + list(range(seqs))
        part_copy(z).wait_recv()
        for i in order:
            start = i * size
            value = own_sum(z, i)
            for d in (DOWN, UP):
                rs_copy(nz // 2 - 1, d, i).wait_recv()
                value = value + sums[d, nz // 2, start:start + size, :].astype(F32)
            states[z, start:start + size, :] = (value * (1.0 / count)).astype(BF16)
            if i == pieces - 1:
                mass = own_mass(z)
                for d in (DOWN, UP):
                    old = sums[d, nz // 2, state_rows:, :].astype(F32)
                    mass = mass + old[:8] + old[8:]
                states[z, state_rows:, :] = split(mass * (1.0 / count))
            ag_copy(0, UP, i).start()
            ag_copy(0, DOWN, i).start()
            if i == pieces - 1:
                hand_copy(z).start()

        def pass_on(k, both, work):
            for slot, i in enumerate(order):
                if both:
                    for d in (early, 1 - early):
                        ag_arrived(k - 1, d, i)
                        ag_copy(k, d, i).start()
                else:
                    for d in (UP, DOWN):
                        ag_arrived(k - 1, d, i)
                    ag_copy(k, 1 - first_way(i), i).start()
                if i == pieces - 1:
                    hand_copy(head_at(-k)).start()
                    hand_copy(head_at(k)).start()
                work(k, slot)

        def weights_here():
            own_load.wait()
            for offset in range(nx * ny):
                piece = lax.rem(chip + offset, nx * ny)
                push_copy(piece, 0).wait_recv()
                if offset > 0:
                    push_copy(piece, 1).wait_recv()

        def read_slice(k, slot):
            read_part(head_at(-k) if slot < seqs else head_at(k), 0, slot % seqs)

        def project_slice(k, slot):
            project_part(head_at(-k), head_at(k), slot)

        def drain(k, slot):
            i = slot
            for d in (UP, DOWN):
                rs_copy(k, d, i).wait_send()

        def first_work(k, slot):
            drain(k, slot)
            if slot < seqs:
                read_part(z, 0, slot)

        def second_work(k, slot):
            drain(k, slot)
            read_slice(k - 1, slot)

        def later_work(k, slot):
            drain(k, slot)
            read_slice(k - 1, slot)
            project_slice(k - 2, slot)

        end = nz // 2
        pass_on(1, True, first_work)
        pass_on(2, True, second_work)
        weights_here()

        @pl.loop(3, end - 1)
        def _(k):
            pass_on(k, True, later_work)
            for i in range(pieces):
                for d in (UP, DOWN):
                    ag_copy(k - 3, d, i).wait_send()

        pass_on(end - 1, False, later_work)
        for slot in range(pieces):
            read_slice(end - 1, slot)
            project_slice(end - 2, slot)
        own_copy().wait_send()
        for k in (end - 4, end - 3):
            for i in range(pieces):
                for d in (UP, DOWN):
                    ag_copy(k, d, i).wait_send()
        for slot, i in enumerate(order):
            ag_arrived(end - 1, 1 - first_way(i), i)
            if i == pieces - 1:
                hand_copy(head_at(end)).start()
            if slot < seqs:
                for part_at in (2 * slot, 2 * slot + 1):
                    project_slice(end - 1, part_at)
            else:
                read_part(head_at(end), 0, slot - seqs)
        project(z, head_at(end), last=True)

        for i in range(pieces):
            rs_copy(0, first_way(i), i).wait_send()
            for d in (UP, DOWN):
                ag_copy(end - 2, d, i).wait_send()
            ag_copy(end - 1, 1 - first_way(i), i).wait_send()

        @pl.loop(0, nz)
        def _(j):
            hand_copy(j).wait_send()

    @pl.when(core == 0)
    def _weights():
        start_loads()
        east, west = y * nx + lax.rem(x + 1, nx), y * nx + lax.rem(x + nx - 1, nx)
        north, south = lax.rem(y + 1, ny) * nx + x, lax.rem(y + ny - 1, ny) * nx + x
        ways = ((east, west), (north, south))
        for device in (east, west, north, south):
            pl.semaphore_signal(barrier, inc=1, device_id={"fsdp": device * 2}, device_id_type=MESH)
        pl.semaphore_signal(barrier, inc=1, device_id=partner, device_id_type=MESH)

        items = (((0, 0), (1, 0), (1, -1), (1, 1), (1, 2)), ((1, 0), (0, 0), (0, -1), (0, 1), (0, 2)))

        def piece_at(axis, item, along):
            across = items[axis][item][1]
            dx, dy = (along, across) if axis == 0 else (across, along)
            return lax.rem(y + dy + ny, ny) * nx + lax.rem(x + dx + nx, nx)

        def line_copy(axis, item, way, stage, arriving):
            sign = 1 if way == 0 else -1
            if stage == 0:
                along, start, rows = 0, 0, half
            else:
                along, start, rows = -sign, way * (half // 2), half // 2
            if arriving:
                along = along - sign
                along = 2 if along == -2 else along
            spot = weight.at[piece_at(axis, item, along), pl.ds(items[axis][item][0] * half + start, rows)]
            return pltpu.make_async_remote_copy(
                spot, spot, line_send.at[axis, item, way, stage], line_recv.at[axis, item, way, stage],
                device_id={"fsdp": ways[axis][way] * 2}, device_id_type=MESH,
            )

        def send(axis, item):
            for way in (0, 1):
                line_copy(axis, item, way, 0, False).start()

        def got(axis, item, stage):
            for way in (0, 1):
                line_copy(axis, item, way, stage, True).wait_recv()

        def forward(axis, item):
            for way in (0, 1):
                line_copy(axis, item, way, 0, True).wait_recv()
                line_copy(axis, item, way, 1, False).start()

        def at(dx, dy):
            return lax.rem(y + dy + ny, ny) * nx + lax.rem(x + dx + nx, nx)

        def push(dx, dy, which):
            push_copy(at(dx, dy), which).start()

        relayout_first()
        partial(head_at(nz // 2), seqs)
        pl.semaphore_wait(barrier, 5)
        part_copy(head_at(nz // 2)).start()
        relayout_rest()

        def part_out(offset):
            partial(head_at(offset), seqs)
            part_copy(head_at(offset)).start()

        part_out(nz // 2 + 1)
        part_out(nz // 2 - 1)
        own_load.wait()
        send(0, 0)
        send(1, 1)

        @pl.loop(2, nz // 2)
        def _(k):
            part_out(nz // 2 + k)
            part_out(nz // 2 - k)

            @pl.when(k == 3)
            def _():
                own_copy().wait_recv()
                send(1, 0)
                send(0, 1)

        part_out(0)
        push(0, 0, 0)
        for load in late_loads:
            load.wait()

        @pl.loop(0, late_units // 2)
        def _(i):
            relayout_late(i)

        forward(0, 0)
        send(1, 2)
        send(1, 3)
        push(-1, 0, 0)
        push(1, 0, 0)
        forward(1, 0)
        send(0, 2)
        send(0, 3)
        push(0, -1, 1)
        push(0, 1, 1)

        @pl.loop(late_units // 2, late_units)
        def _(i):
            relayout_late(i)

        forward(0, 1)
        forward(1, 1)
        push(-1, 0, 1)
        push(1, 0, 1)
        push(0, -1, 0)
        push(0, 1, 0)
        got(0, 0, 1)
        send(1, 4)
        push(2, 0, 0)
        got(1, 0, 1)
        send(0, 4)
        push(0, 2, 1)
        for item, off in ((2, -1), (3, 1)):
            forward(1, item)
            push(off, -1, 0)
            push(off, 1, 0)
            forward(0, item)
            push(-1, off, 1)
            push(1, off, 1)
        got(0, 1, 1)
        push(2, 0, 1)
        got(1, 1, 1)
        push(0, 2, 0)
        forward(1, 4)
        push(2, -1, 0)
        push(2, 1, 0)
        forward(0, 4)
        push(-1, 2, 1)
        push(1, 2, 1)
        for item, off in ((2, -1), (3, 1), (4, 2)):
            got(1, item, 1)
            push(off, 2, 0)
            got(0, item, 1)
            push(2, off, 1)

        for axis in (0, 1):
            for item in range(5):
                for way in (0, 1):
                    for stage in (0, 1):
                        line_copy(axis, item, way, stage, False).wait_send()

        @pl.loop(0, nz)
        def _(j):
            part_copy(j).wait_send()

        hand_copy(z).wait_recv()
        read_head(z, seqs)

        def read_pair(k):
            for head in (head_at(-k), head_at(k)):
                hand_copy(head).wait_recv()
                read_head(head, seqs)

        read_pair(1)
        project(head_at(-1), head_at(1), first=True)
        for offset in range(nx * ny):
            piece = lax.rem(chip + offset, nx * ny)
            push_copy(piece, 0).wait_send()
            if offset > 0:
                push_copy(piece, 1).wait_send()

        @pl.loop(2, nz // 2)
        def _(k):
            read_pair(k)
            project(head_at(-k), head_at(k))

        hand_copy(head_at(nz // 2)).wait_recv()
        read_head(head_at(nz // 2), seqs)
        project(z, head_at(nz // 2), last=True)


def local(ny, nx, nz, query_rows, key_rows, value_rows, gate_rows, out_weight):
    seqs, tokens, heads, size = query_rows.shape
    rows, width = out_weight.shape
    chips = nx * ny
    raw = pltpu.VMEM((seqs, tokens, heads, size), BF16)
    split = pltpu.VMEM((heads, seqs, tokens, size), BF16)
    part = pltpu.VMEM((heads, seqs * size + 8, size), F32)
    chunk = 2 * seqs * size + 16
    dma = pltpu.SemaphoreType.DMA
    return pl.pallas_call(
        functools.partial(layer_kernel, ny, nx, nz, float(tokens * nz)),
        name="layer",
        out_shape=jax.ShapeDtypeStruct((seqs, tokens, width), BF16),
        in_specs=[pl.BlockSpec(memory_space=pltpu.HBM)] * 5,
        out_specs=pl.BlockSpec(memory_space=pltpu.VMEM),
        scratch_shapes=[
            raw, raw, raw, raw,
            split, split, split,
            pltpu.VMEM((heads, seqs, tokens, size), F32),
            part, part,
            pltpu.VMEM((2, nz // 2 + 1, chunk, size), BF16),
            pltpu.VMEM((heads, chunk, size), BF16),
            pltpu.VMEM((chips, 2 * rows, width), BF16),
            pltpu.VMEM((heads, seqs * tokens, size), BF16),
            pltpu.VMEM((seqs * tokens, width), F32),
            dma((4, seqs)),
            dma((heads,)), dma((heads,)),
            dma((nz // 2, 2, 2 * seqs)), dma((nz // 2, 2, 2 * seqs)),
            dma((nz // 2, 2, 2 * seqs)), dma((nz // 2, 2, 2 * seqs)),
            dma((heads,)), dma((heads,)),
            dma((2, 5, 2, 2)), dma((2, 5, 2, 2)),
            dma((chips, 2)), dma((chips, 2)),
            dma, dma,
        ],
        compiler_params=pltpu.CompilerParams(
            collective_id=0, has_side_effects=True, vmem_limit_bytes=52 * 2**20
        ),
    )(query_rows, key_rows, value_rows, gate_rows, pltpu.with_memory_space_constraint(out_weight, pltpu.HBM))


def solution(mesh):
    in_specs = (
        P("fsdp", "seq", None, None),
        P("fsdp", "seq", None, None),
        P("fsdp", "seq", None, None),
        P("fsdp", "seq", None, None),
        P("fsdp", None),
    )
    out_specs = P("fsdp", "seq", None)
    body = functools.partial(local, 4, 4, mesh.shape["seq"])
    return jax.shard_map(body, mesh=mesh, in_specs=in_specs, out_specs=out_specs, check_vma=False)
```

```python
import functools

import jax
import jax.numpy as jnp
from jax import lax
from jax.experimental import pallas as pl
from jax.experimental.pallas import tpu as pltpu
from jax.sharding import PartitionSpec as P

MESH = pl.DeviceIdType.MESH
F32, BF16 = jnp.float32, jnp.bfloat16
BLOCK = 32
UP, DOWN = 0, 1
SIDE_FAR, SIDE_NEAR = 6, 7
HOPS = (1, 1, 1, 1, 2, 2, 1, 1)
ROLES = (8, 7, 6, 5, 4, 2, 3, 1)
AG_HOPS = (2, 2, 1, 1, 1, 1, 1, 1)
HELD = (0, 2, 4, 5, 6, 7, 2, 0)


def feature(raw):
    wide = raw.astype(F32)
    return wide * wide + 0.1


def layer_kernel(
    ny, nx, nz, count,
    q_hbm, k_hbm, v_hbm, g_hbm, w_hbm, out_ref,
    q_raw, k_raw, v_raw, g_raw, q_feat, k_feat, v_head, gates,
    part, other, sums, states, weight, mixed, total,
    load_sem, part_send, part_recv, rs_send, rs_recv, ag_send, ag_recv,
    hand_send, hand_recv, line_send, line_recv, push_send, push_recv, own_send, own_recv,
):
    seqs, tokens, heads, size = k_raw.shape
    width = weight.shape[2]
    half = weight.shape[1] // 2
    state_rows = 2 * seqs * size
    z, f = lax.axis_index("seq"), lax.axis_index("fsdp")
    core = lax.rem(f, 2)
    chip = f // 2
    x, y = lax.rem(chip, nx), chip // nx
    partner = {"fsdp": chip * 2 + 1 - core}
    barrier = pltpu.get_barrier_semaphore()

    def head_at(offset):
        return lax.rem(z + offset + 2 * nz, nz)

    key_loads, value_loads = (
        [pltpu.make_async_copy(src.at[s], dst.at[s], load_sem.at[at, s]) for s in range(seqs)]
        for at, (src, dst) in enumerate(((k_hbm, k_raw), (v_hbm, v_raw)))
    )
    late_loads = [
        pltpu.make_async_copy(src, dst, load_sem.at[2, at])
        for at, (src, dst) in enumerate(((q_hbm, q_raw), (g_hbm, g_raw)))
    ]
    own_rows = weight.at[chip, pl.ds(pl.multiple_of(core * half, half), half)]
    own_load = pltpu.make_async_copy(w_hbm, own_rows, load_sem.at[3, 0])

    def start_loads():
        for s in range(seqs):
            key_loads[s].start()
            value_loads[s].start()
        own_load.start()
        for load in late_loads:
            load.start()

    def by_head(values):
        return jnp.swapaxes(values, 0, 1)

    group = heads // 2

    def relayout(which, wait):
        span = slice(which * group, (which + 1) * group)
        for s in range(seqs):
            for load, src, dst, fn in (
                (key_loads[s], k_raw, k_feat, feature),
                (value_loads[s], v_raw, v_head, lambda raw: raw.astype(F32)),
            ):
                if wait:
                    load.wait()

                @pl.loop(0, tokens // BLOCK)
                def _(i):
                    rows = pl.ds(pl.multiple_of(i * BLOCK, BLOCK), BLOCK)
                    dst[span, s, rows, :] = by_head(fn(src[s, rows, span])).astype(BF16)

    def partials(which):
        first_row = seqs * (1 - core)
        ones = jnp.ones((8, tokens), BF16)
        place = lax.broadcasted_iota(jnp.int32, (8, size), 0)
        for head in range(which * group, (which + 1) * group):
            mass = jnp.zeros((8, size), F32)
            for s in range(seqs):
                keys = k_feat[head, s]
                part[head, s * size:(s + 1) * size, :] = lax.dot_general(
                    keys, v_head[head, s], (((0,), (0,)), ((), ())), preferred_element_type=F32
                )
                row = jnp.dot(ones, keys, preferred_element_type=F32)
                mass = jnp.where(place == first_row + s, row, mass)
            part[head, seqs * size:, :] = mass

    starts_late = z >= nz // 2

    def prepare_first():
        relayout(0, True)
        partials(0)

        @pl.when(jnp.logical_not(starts_late))
        def _():
            relayout(1, False)
            partials(1)

    def prepare_rest():
        @pl.when(starts_late)
        def _():
            relayout(1, False)
            partials(1)

    def relayout_late(unit):
        per_seq = tokens // BLOCK
        s = unit // per_seq
        rows = pl.ds(pl.multiple_of(lax.rem(unit, per_seq) * BLOCK, BLOCK), BLOCK)
        q_feat[:, s, rows, :] = by_head(feature(q_raw[s, rows])).astype(BF16)
        gate = g_raw[s, rows].astype(F32)
        gates[:, s, rows, :] = by_head(count**0.5 / (1.0 + jnp.exp(-gate)))

    late_units = seqs * tokens // BLOCK

    def read_part(head, first_row, s):
        tail = states[head, state_rows:, :].astype(F32)
        row = first_row + s
        feats = q_feat[head, s]
        top = jnp.dot(feats, states[head, row * size:(row + 1) * size, :], preferred_element_type=F32)
        mass = tail[row:row + 1] + tail[8 + row:9 + row]
        bottom = jnp.sum(feats.astype(F32) * mass, axis=1, keepdims=True)
        read = top * (1.0 / (bottom + 0.001))
        mixed[head, s * tokens:(s + 1) * tokens, :] = (read * gates[head, s]).astype(BF16)

    def read_head(head, first_row):
        for s in range(seqs):
            read_part(head, first_row, s)

    step = width // 4

    def project_part(a, b, i, first=False, last=False):
        rows = jnp.concatenate([mixed[a], mixed[b]], axis=1)
        cols = pl.ds(i * step, step)
        piece = jnp.dot(
            rows, jnp.concatenate([weight[a, :, cols], weight[b, :, cols]], axis=0),
            preferred_element_type=F32,
        )
        if not first:
            piece = total[:, cols] + piece
        if last:
            for s in range(seqs):
                out_ref[s, :, cols] = piece[s * tokens:(s + 1) * tokens].astype(BF16)
        else:
            total[:, cols] = piece

    def project(a, b, first=False, last=False):
        for i in range(width // step):
            project_part(a, b, i, first, last)

    def part_copy(head):
        return pltpu.make_async_remote_copy(
            part.at[head], other.at[head], part_send.at[head], part_recv.at[head],
            device_id=partner, device_id_type=MESH,
        )

    def hand_copy(head):
        rows = pl.ds(seqs * size, state_rows + 16 - seqs * size)
        return pltpu.make_async_remote_copy(
            states.at[head, rows], states.at[head, rows], hand_send.at[head], hand_recv.at[head],
            device_id=partner, device_id_type=MESH,
        )

    def push_copy(piece, which):
        rows = pl.ds(which * half, half)
        return pltpu.make_async_remote_copy(
            weight.at[piece, rows], weight.at[piece, rows],
            push_send.at[piece, which], push_recv.at[piece, which],
            device_id=partner, device_id_type=MESH,
        )

    def own_copy():
        return pltpu.make_async_remote_copy(
            w_hbm, weight.at[chip, pl.ds(half, half)], own_send, own_recv,
            device_id=partner, device_id_type=MESH,
        )

    @pl.when(core == 1)
    def _ring():
        start_loads()
        near = [{"seq": lax.rem(z + hop, nz)} for hop in (1, 2, nz - 2, nz - 1)]
        for device in near + [partner]:
            pl.semaphore_signal(barrier, inc=1, device_id=device, device_id_type=MESH)
        prepare_first()
        pl.semaphore_wait(barrier, 5)
        own_copy().start()

        pieces = 2 * seqs
        spans = [(i * size, size if i < pieces - 1 else size + 16) for i in range(pieces)]
        early = jnp.where(lax.rem(z, 4) < 2, DOWN, UP)
        both = (early, 1 - early)

        def target(d, hop):
            return {"seq": lax.rem(z + jnp.where(d == UP, hop, nz - hop), nz)}

        def source(m):
            return m if m < SIDE_FAR else 2 * m - 5

        def rs_copy(m, d, i):
            rows = pl.ds(*spans[i])
            return pltpu.make_async_remote_copy(
                sums.at[d, source(m), rows], sums.at[d, source(m) + 1, rows],
                rs_send.at[m, d, i], rs_recv.at[m, d, i],
                device_id=target(d, HOPS[m]), device_id_type=MESH,
            )

        def ag_message(m, d, i, distance):
            rows = pl.ds(*spans[i])
            head = head_at(jnp.where(d == UP, -distance, distance))
            return pltpu.make_async_remote_copy(
                states.at[head, rows], states.at[head, rows], ag_send.at[m, d, i], ag_recv.at[m, d, i],
                device_id=target(d, AG_HOPS[m]), device_id_type=MESH,
            )

        def ag_copy(m, d, i):
            return ag_message(m, d, i, HELD[m])

        def ag_arrived(m, d, i):
            ag_message(m, d, i, HELD[m] + AG_HOPS[m]).wait_recv()

        def own_sum(head, i):
            if i < seqs:
                return part[head, i * size:(i + 1) * size, :]
            return other[head, (i - seqs) * size:(i - seqs + 1) * size, :]

        def own_mass(head):
            return part[head, seqs * size:, :] + other[head, seqs * size:, :]

        def split(mass):
            high = mass.astype(BF16)
            return jnp.concatenate([high.astype(F32), mass - high.astype(F32)], axis=0).astype(BF16)

        def add_and_send(m, d, i, received=()):
            head = head_at(jnp.where(d == UP, ROLES[m], -ROLES[m]))
            start = i * size
            slot = source(m)
            value = own_sum(head, i)
            for r in received:
                rs_copy(r, d, i).wait_recv()
                value = value + sums[d, source(r) + 1, start:start + size, :].astype(F32)
            sums[d, slot, start:start + size, :] = value.astype(BF16)
            if i == pieces - 1:
                mass = own_mass(head)
                for r in received:
                    old = sums[d, source(r) + 1, state_rows:, :].astype(F32)
                    mass = mass + old[:8] + old[8:]
                sums[d, slot, state_rows:, :] = split(mass)
            rs_copy(m, d, i).start()

        def first_way(i):
            return DOWN if i < seqs else UP

        def other_here(m):
            part_copy(head_at(ROLES[m])).wait_recv()
            part_copy(head_at(-ROLES[m])).wait_recv()

        def side(m, some):
            for i in some:
                if i == seqs:
                    other_here(m)
                for d in both:
                    add_and_send(m, d, i)

        own_half, other_half = range(seqs), range(seqs, pieces)

        for i in range(pieces):
            if i == seqs:
                part_copy(head_at(nz // 2)).wait_recv()
            add_and_send(0, first_way(i), i)
        prepare_rest()
        for i in range(pieces):
            if i == seqs:
                other_here(1)
            add_and_send(1, 1 - first_way(i), i)
            add_and_send(1, first_way(i), i, (0,))
        side(SIDE_FAR, own_half)
        for load in late_loads:
            load.wait()
        sides = {2: (SIDE_FAR, other_half), 3: (SIDE_NEAR, own_half), 4: (SIDE_NEAR, other_half)}
        for m in range(2, 6):
            for i in range(pieces):
                if i == seqs:
                    other_here(m)
                for d in both:
                    add_and_send(m, d, i, (m - 1, SIDE_FAR) if m == 5 else (m - 1,))
            if m in sides:
                side(*sides[m])

            @pl.loop((m - 2) * late_units // 4, (m - 1) * late_units // 4)
            def _(unit):
                relayout_late(unit)

        order = list(other_half) + list(own_half)
        part_copy(z).wait_recv()
        for i in order:
            start = i * size
            value = own_sum(z, i)
            for m, d in ((SIDE_NEAR, DOWN), (SIDE_NEAR, UP), (5, DOWN), (5, UP)):
                rs_copy(m, d, i).wait_recv()
                value = value + sums[d, source(m) + 1, start:start + size, :].astype(F32)
            states[z, start:start + size, :] = (value * (1.0 / count)).astype(BF16)
            if i == pieces - 1:
                mass = own_mass(z)
                for m in (SIDE_NEAR, 5):
                    for d in (DOWN, UP):
                        old = sums[d, source(m) + 1, state_rows:, :].astype(F32)
                        mass = mass + old[:8] + old[8:]
                states[z, state_rows:, :] = split(mass * (1.0 / count))
            ag_copy(0, UP, i).start()
            ag_copy(0, DOWN, i).start()
            if i == pieces - 1:
                hand_copy(z).start()

        def hand_pair(distance):
            hand_copy(head_at(-distance)).start()
            hand_copy(head_at(distance)).start()

        def pass_on(m, work, extra=None):
            for slot, i in enumerate(order):
                if m < 5:
                    for d in both:
                        ag_arrived(m - 1, d, i)
                        ag_copy(m, d, i).start()
                else:
                    for d in (UP, DOWN):
                        ag_arrived(m - 1, d, i)
                    ag_copy(m, 1 - first_way(i), i).start()
                if i == pieces - 1:
                    hand_pair(HELD[m])
                for d in (UP, DOWN):
                    rs_copy(m, d, i).wait_send()
                if slot < pieces - 1:
                    work(slot)
            if extra is not None:
                for i in extra[1]:
                    for d in both:
                        ag_copy(extra[0], d, i).start()
            work(pieces - 1)

        def side_came(m):
            for i in order:
                for d in both:
                    ag_arrived(m, d, i)
                if i == pieces - 1:
                    hand_pair(HELD[m] + AG_HOPS[m])

        def gone(*messages):
            for m in messages:
                for i in range(pieces):
                    for d in (UP, DOWN):
                        ag_copy(m, d, i).wait_send()

        def weights_here():
            own_load.wait()
            for offset in range(nx * ny):
                piece = lax.rem(chip + offset, nx * ny)
                push_copy(piece, 0).wait_recv()
                if offset > 0:
                    push_copy(piece, 1).wait_recv()

        def read_slice(distance, slot):
            read_part(head_at(-distance) if slot < seqs else head_at(distance), 0, slot % seqs)

        def project_slice(distance, slot, first=False):
            project_part(head_at(-distance), head_at(distance), slot, first)

        def work_1(slot):
            if slot < seqs:
                read_part(z, 0, slot)

        def work_2(slot):
            read_slice(2, slot)

        def work_3(slot):
            read_slice(4, slot)

        def work_4(slot):
            read_slice(5, slot)
            project_slice(2, slot, True)
            project_slice(4, slot)

        def work_5(slot):
            read_slice(6, slot)
            read_slice(1, slot)
            project_slice(5, slot)

        pass_on(1, work_1, (SIDE_NEAR, other_half))
        pass_on(2, work_2, (SIDE_NEAR, own_half))
        pass_on(3, work_3, (SIDE_FAR, other_half))
        weights_here()
        pass_on(4, work_4, (SIDE_FAR, own_half))
        side_came(SIDE_NEAR)
        pass_on(5, work_5)
        own_copy().wait_send()
        for slot in range(pieces):
            read_slice(7, slot)
            project_slice(1, slot)
        side_came(SIDE_FAR)
        for slot in range(pieces):
            read_slice(3, slot)
            project_slice(6, slot)
        for i in range(pieces):
            rs_copy(0, first_way(i), i).wait_send()
            for d in (UP, DOWN):
                rs_copy(SIDE_FAR, d, i).wait_send()
                rs_copy(SIDE_NEAR, d, i).wait_send()
        gone(0, 1, 2, SIDE_NEAR)
        end = nz // 2
        for slot, i in enumerate(order):
            ag_arrived(5, 1 - first_way(i), i)
            if i == pieces - 1:
                hand_copy(head_at(end)).start()
            if slot < seqs:
                for part_at in (2 * slot, 2 * slot + 1):
                    project_slice(7, part_at)
                    project_slice(3, part_at)
            else:
                read_part(head_at(end), 0, slot - seqs)
        project(z, head_at(end), last=True)

        gone(3, 4, SIDE_FAR)
        for i in range(pieces):
            ag_copy(5, 1 - first_way(i), i).wait_send()

        @pl.loop(0, nz)
        def _(j):
            hand_copy(j).wait_send()

    @pl.when(core == 0)
    def _weights():
        start_loads()
        east, west = y * nx + lax.rem(x + 1, nx), y * nx + lax.rem(x + nx - 1, nx)
        north, south = lax.rem(y + 1, ny) * nx + x, lax.rem(y + ny - 1, ny) * nx + x
        ways = ((east, west), (north, south))
        for device in (east, west, north, south):
            pl.semaphore_signal(barrier, inc=1, device_id={"fsdp": device * 2}, device_id_type=MESH)
        pl.semaphore_signal(barrier, inc=1, device_id=partner, device_id_type=MESH)

        items = (((0, 0), (1, 0), (1, -1), (1, 1), (1, 2)), ((1, 0), (0, 0), (0, -1), (0, 1), (0, 2)))

        def piece_at(axis, item, along):
            across = items[axis][item][1]
            dx, dy = (along, across) if axis == 0 else (across, along)
            return lax.rem(y + dy + ny, ny) * nx + lax.rem(x + dx + nx, nx)

        def line_copy(axis, item, way, stage, arriving):
            sign = 1 if way == 0 else -1
            if stage == 0:
                along, start, rows = 0, 0, half
            else:
                along, start, rows = -sign, way * (half // 2), half // 2
            if arriving:
                along = along - sign
                along = 2 if along == -2 else along
            spot = weight.at[piece_at(axis, item, along), pl.ds(items[axis][item][0] * half + start, rows)]
            return pltpu.make_async_remote_copy(
                spot, spot, line_send.at[axis, item, way, stage], line_recv.at[axis, item, way, stage],
                device_id={"fsdp": ways[axis][way] * 2}, device_id_type=MESH,
            )

        def send(axis, item):
            for way in (0, 1):
                line_copy(axis, item, way, 0, False).start()

        def got(axis, item, stage):
            for way in (0, 1):
                line_copy(axis, item, way, stage, True).wait_recv()

        def forward(axis, item):
            for way in (0, 1):
                line_copy(axis, item, way, 0, True).wait_recv()
                line_copy(axis, item, way, 1, False).start()

        def at(dx, dy):
            return lax.rem(y + dy + ny, ny) * nx + lax.rem(x + dx + nx, nx)

        def push(dx, dy, which):
            push_copy(at(dx, dy), which).start()

        prepare_first()
        pl.semaphore_wait(barrier, 5)
        part_copy(head_at(nz // 2)).start()
        prepare_rest()

        part_order = (7, 3, 6, 5, 1, 4, 2)
        for distance in part_order[:2]:
            part_copy(head_at(-distance)).start()
            part_copy(head_at(distance)).start()
        own_load.wait()
        send(0, 0)
        send(1, 1)
        for distance in part_order[2:]:
            part_copy(head_at(-distance)).start()
            part_copy(head_at(distance)).start()
        part_copy(z).start()
        own_copy().wait_recv()
        send(1, 0)
        send(0, 1)
        push(0, 0, 0)
        for load in late_loads:
            load.wait()

        @pl.loop(0, late_units // 2)
        def _(i):
            relayout_late(i)

        forward(0, 0)
        send(1, 2)
        send(1, 3)
        push(-1, 0, 0)
        push(1, 0, 0)
        forward(1, 0)
        send(0, 2)
        send(0, 3)
        push(0, -1, 1)
        push(0, 1, 1)

        @pl.loop(late_units // 2, late_units)
        def _(i):
            relayout_late(i)

        forward(0, 1)
        forward(1, 1)
        push(-1, 0, 1)
        push(1, 0, 1)
        push(0, -1, 0)
        push(0, 1, 0)
        got(0, 0, 1)
        send(1, 4)
        push(2, 0, 0)
        got(1, 0, 1)
        send(0, 4)
        push(0, 2, 1)
        for item, off in ((2, -1), (3, 1)):
            forward(1, item)
            push(off, -1, 0)
            push(off, 1, 0)
            forward(0, item)
            push(-1, off, 1)
            push(1, off, 1)
        got(0, 1, 1)
        push(2, 0, 1)
        got(1, 1, 1)
        push(0, 2, 0)
        forward(1, 4)
        push(2, -1, 0)
        push(2, 1, 0)
        forward(0, 4)
        push(-1, 2, 1)
        push(1, 2, 1)
        for item, off in ((2, -1), (3, 1), (4, 2)):
            got(1, item, 1)
            push(off, 2, 0)
            got(0, item, 1)
            push(2, off, 1)

        for axis in (0, 1):
            for item in range(5):
                for way in (0, 1):
                    for stage in (0, 1):
                        line_copy(axis, item, way, stage, False).wait_send()

        @pl.loop(0, nz)
        def _(j):
            part_copy(j).wait_send()

        hand_copy(z).wait_recv()
        read_head(z, seqs)

        def read_pair(k):
            for head in (head_at(-k), head_at(k)):
                hand_copy(head).wait_recv()
                read_head(head, seqs)

        read_pair(2)
        project(head_at(-2), head_at(2), first=True)
        for offset in range(nx * ny):
            piece = lax.rem(chip + offset, nx * ny)
            push_copy(piece, 0).wait_send()
            if offset > 0:
                push_copy(piece, 1).wait_send()

        for k in (4, 5, 1, 6, 7, 3):
            read_pair(k)
            project(head_at(-k), head_at(k))

        hand_copy(head_at(nz // 2)).wait_recv()
        read_head(head_at(nz // 2), seqs)
        project(z, head_at(nz // 2), last=True)


def local(ny, nx, nz, query_rows, key_rows, value_rows, gate_rows, out_weight):
    seqs, tokens, heads, size = query_rows.shape
    rows, width = out_weight.shape
    chips = nx * ny
    raw = pltpu.VMEM((seqs, tokens, heads, size), BF16)
    split = pltpu.VMEM((heads, seqs, tokens, size), BF16)
    part = pltpu.VMEM((heads, seqs * size + 8, size), F32)
    chunk = 2 * seqs * size + 16
    dma = pltpu.SemaphoreType.DMA
    return pl.pallas_call(
        functools.partial(layer_kernel, ny, nx, nz, float(tokens * nz)),
        name="layer",
        out_shape=jax.ShapeDtypeStruct((seqs, tokens, width), BF16),
        in_specs=[pl.BlockSpec(memory_space=pltpu.HBM)] * 5,
        out_specs=pl.BlockSpec(memory_space=pltpu.VMEM),
        scratch_shapes=[
            raw, raw, raw, raw,
            split, split, split,
            pltpu.VMEM((heads, seqs, tokens, size), F32),
            part, part,
            pltpu.VMEM((2, 11, chunk, size), BF16),
            pltpu.VMEM((heads, chunk, size), BF16),
            pltpu.VMEM((chips, 2 * rows, width), BF16),
            pltpu.VMEM((heads, seqs * tokens, size), BF16),
            pltpu.VMEM((seqs * tokens, width), F32),
            dma((4, seqs)),
            dma((heads,)), dma((heads,)),
            dma((8, 2, 2 * seqs)), dma((8, 2, 2 * seqs)),
            dma((8, 2, 2 * seqs)), dma((8, 2, 2 * seqs)),
            dma((heads,)), dma((heads,)),
            dma((2, 5, 2, 2)), dma((2, 5, 2, 2)),
            dma((chips, 2)), dma((chips, 2)),
            dma, dma,
        ],
        compiler_params=pltpu.CompilerParams(
            collective_id=0, has_side_effects=True, vmem_limit_bytes=52 * 2**20
        ),
    )(query_rows, key_rows, value_rows, gate_rows, pltpu.with_memory_space_constraint(out_weight, pltpu.HBM))


def solution(mesh):
    in_specs = (
        P("fsdp", "seq", None, None),
        P("fsdp", "seq", None, None),
        P("fsdp", "seq", None, None),
        P("fsdp", "seq", None, None),
        P("fsdp", None),
    )
    out_specs = P("fsdp", "seq", None)
    body = functools.partial(local, 4, 4, mesh.shape["seq"])
    return jax.shard_map(body, mesh=mesh, in_specs=in_specs, out_specs=out_specs, check_vma=False)
```

```python
import functools

import jax
import jax.numpy as jnp
from jax import lax
from jax.experimental import pallas as pl
from jax.experimental.pallas import tpu as pltpu
from jax.sharding import PartitionSpec as P

MESH = pl.DeviceIdType.MESH
F32, BF16 = jnp.float32, jnp.bfloat16
BLOCK = 32
UP, DOWN = 0, 1
SIDE_FAR, SIDE_NEAR = 6, 7
HOPS = (1, 1, 1, 1, 2, 2, 1, 1)
ROLES = (8, 7, 6, 5, 4, 2, 3, 1)
AG_HOPS = (2, 2, 1, 1, 1, 1, 1, 1)
HELD = (0, 2, 4, 5, 6, 7, 2, 0)


def feature(raw):
    wide = raw.astype(F32)
    return wide * wide + 0.1


def layer_kernel(
    ny, nx, nz, count,
    q_hbm, k_hbm, v_hbm, g_hbm, w_hbm, out_ref,
    q_raw, k_raw, v_raw, g_raw, q_feat, k_feat, v_head, gates,
    part, other, sums, states, weight, mixed, total,
    load_sem, part_send, part_recv, rs_send, rs_recv, ag_send, ag_recv,
    hand_send, hand_recv, line_send, line_recv, push_send, push_recv, own_send, own_recv,
):
    seqs, tokens, heads, size = k_raw.shape
    width = weight.shape[2]
    half = weight.shape[1] // 2
    state_rows = 2 * seqs * size
    z, f = lax.axis_index("seq"), lax.axis_index("fsdp")
    core = lax.rem(f, 2)
    chip = f // 2
    x, y = lax.rem(chip, nx), chip // nx
    partner = {"fsdp": chip * 2 + 1 - core}
    barrier = pltpu.get_barrier_semaphore()

    def head_at(offset):
        return lax.rem(z + offset + 2 * nz, nz)

    key_loads, value_loads = (
        [pltpu.make_async_copy(src.at[s], dst.at[s], load_sem.at[at, s]) for s in range(seqs)]
        for at, (src, dst) in enumerate(((k_hbm, k_raw), (v_hbm, v_raw)))
    )
    late_loads = [
        pltpu.make_async_copy(src, dst, load_sem.at[2, at])
        for at, (src, dst) in enumerate(((q_hbm, q_raw), (g_hbm, g_raw)))
    ]
    own_rows = weight.at[chip, pl.ds(pl.multiple_of(core * half, half), half)]
    own_load = pltpu.make_async_copy(w_hbm, own_rows, load_sem.at[3, 0])

    def start_loads():
        for s in range(seqs):
            key_loads[s].start()
            value_loads[s].start()
        own_load.start()
        for load in late_loads:
            load.start()

    def by_head(values):
        return jnp.swapaxes(values, 0, 1)

    group = heads // 2

    def relayout(which, wait):
        span = slice(which * group, (which + 1) * group)
        for s in range(seqs):
            for load, src, dst, fn in (
                (key_loads[s], k_raw, k_feat, feature),
                (value_loads[s], v_raw, v_head, lambda raw: raw.astype(F32)),
            ):
                if wait:
                    load.wait()

                @pl.loop(0, tokens // BLOCK)
                def _(i):
                    rows = pl.ds(pl.multiple_of(i * BLOCK, BLOCK), BLOCK)
                    dst[span, s, rows, :] = by_head(fn(src[s, rows, span])).astype(BF16)

    def partials(which):
        first_row = seqs * (1 - core)
        ones = jnp.ones((8, tokens), BF16)
        place = lax.broadcasted_iota(jnp.int32, (8, size), 0)
        for head in range(which * group, (which + 1) * group):
            mass = jnp.zeros((8, size), F32)
            for s in range(seqs):
                keys = k_feat[head, s]
                part[head, s * size:(s + 1) * size, :] = lax.dot_general(
                    keys, v_head[head, s], (((0,), (0,)), ((), ())), preferred_element_type=F32
                )
                row = jnp.dot(ones, keys, preferred_element_type=F32)
                mass = jnp.where(place == first_row + s, row, mass)
            part[head, seqs * size:, :] = mass

    starts_late = z >= nz // 2

    def prepare_first():
        relayout(0, True)
        partials(0)

        @pl.when(jnp.logical_not(starts_late))
        def _():
            relayout(1, False)
            partials(1)

    def prepare_rest():
        @pl.when(starts_late)
        def _():
            relayout(1, False)
            partials(1)

    def relayout_late(unit):
        per_seq = tokens // BLOCK
        s = unit // per_seq
        rows = pl.ds(pl.multiple_of(lax.rem(unit, per_seq) * BLOCK, BLOCK), BLOCK)
        q_feat[:, s, rows, :] = by_head(feature(q_raw[s, rows])).astype(BF16)
        gate = g_raw[s, rows].astype(F32)
        gates[:, s, rows, :] = by_head(count**0.5 / (1.0 + jnp.exp(-gate)))

    late_units = seqs * tokens // BLOCK

    def read_part(head, first_row, s):
        tail = states[head, state_rows:, :].astype(F32)
        row = first_row + s
        feats = q_feat[head, s]
        top = jnp.dot(feats, states[head, row * size:(row + 1) * size, :], preferred_element_type=F32)
        mass = tail[row:row + 1] + tail[8 + row:9 + row]
        bottom = jnp.sum(feats.astype(F32) * mass, axis=1, keepdims=True)
        read = top * (1.0 / (bottom + 0.001))
        mixed[head, s * tokens:(s + 1) * tokens, :] = (read * gates[head, s]).astype(BF16)

    def read_head(head, first_row):
        for s in range(seqs):
            read_part(head, first_row, s)

    step = width // 4

    def project_part(a, b, i, first=False, last=False):
        rows = jnp.concatenate([mixed[a], mixed[b]], axis=1)
        cols = pl.ds(i * step, step)
        piece = jnp.dot(
            rows, jnp.concatenate([weight[a, :, cols], weight[b, :, cols]], axis=0),
            preferred_element_type=F32,
        )
        if not first:
            piece = total[:, cols] + piece
        if last:
            for s in range(seqs):
                out_ref[s, :, cols] = piece[s * tokens:(s + 1) * tokens].astype(BF16)
        else:
            total[:, cols] = piece

    def project(a, b, first=False, last=False):
        for i in range(width // step):
            project_part(a, b, i, first, last)

    def part_copy(head):
        return pltpu.make_async_remote_copy(
            part.at[head], other.at[head], part_send.at[head], part_recv.at[head],
            device_id=partner, device_id_type=MESH,
        )

    def hand_copy(head):
        rows = pl.ds(seqs * size, state_rows + 16 - seqs * size)
        return pltpu.make_async_remote_copy(
            states.at[head, rows], states.at[head, rows], hand_send.at[head], hand_recv.at[head],
            device_id=partner, device_id_type=MESH,
        )

    def push_copy(piece, which):
        rows = pl.ds(which * half, half)
        return pltpu.make_async_remote_copy(
            weight.at[piece, rows], weight.at[piece, rows],
            push_send.at[piece, which], push_recv.at[piece, which],
            device_id=partner, device_id_type=MESH,
        )

    def own_copy():
        return pltpu.make_async_remote_copy(
            w_hbm, weight.at[chip, pl.ds(half, half)], own_send, own_recv,
            device_id=partner, device_id_type=MESH,
        )

    @pl.when(core == 1)
    def _ring():
        start_loads()
        near = [{"seq": lax.rem(z + hop, nz)} for hop in (1, 2, nz - 2, nz - 1)]
        for device in near + [partner]:
            pl.semaphore_signal(barrier, inc=1, device_id=device, device_id_type=MESH)
        prepare_first()
        pl.semaphore_wait(barrier, 5)
        own_copy().start()

        pieces = 2 * seqs
        spans = [(i * size, size if i < pieces - 1 else size + 16) for i in range(pieces)]
        early = jnp.where(lax.rem(z, 4) < 2, DOWN, UP)
        both = (early, 1 - early)

        def target(d, hop):
            return {"seq": lax.rem(z + jnp.where(d == UP, hop, nz - hop), nz)}

        def source(m):
            return m if m < SIDE_FAR else 2 * m - 5

        def rs_copy(m, d, i):
            rows = pl.ds(*spans[i])
            return pltpu.make_async_remote_copy(
                sums.at[d, source(m), rows], sums.at[d, source(m) + 1, rows],
                rs_send.at[m, d, i], rs_recv.at[m, d, i],
                device_id=target(d, HOPS[m]), device_id_type=MESH,
            )

        def ag_message(m, d, i, distance):
            rows = pl.ds(*spans[i])
            head = head_at(jnp.where(d == UP, -distance, distance))
            return pltpu.make_async_remote_copy(
                states.at[head, rows], states.at[head, rows], ag_send.at[m, d, i], ag_recv.at[m, d, i],
                device_id=target(d, AG_HOPS[m]), device_id_type=MESH,
            )

        def ag_copy(m, d, i):
            return ag_message(m, d, i, HELD[m])

        def ag_arrived(m, d, i):
            ag_message(m, d, i, HELD[m] + AG_HOPS[m]).wait_recv()

        def own_sum(head, i):
            if i < seqs:
                return part[head, i * size:(i + 1) * size, :]
            return other[head, (i - seqs) * size:(i - seqs + 1) * size, :]

        def own_mass(head):
            return part[head, seqs * size:, :] + other[head, seqs * size:, :]

        def split(mass):
            high = mass.astype(BF16)
            return jnp.concatenate([high.astype(F32), mass - high.astype(F32)], axis=0).astype(BF16)

        def add_and_send(m, d, i, received=()):
            head = head_at(jnp.where(d == UP, ROLES[m], -ROLES[m]))
            start = i * size
            slot = source(m)
            value = own_sum(head, i)
            for r in received:
                rs_copy(r, d, i).wait_recv()
                value = value + sums[d, source(r) + 1, start:start + size, :].astype(F32)
            sums[d, slot, start:start + size, :] = value.astype(BF16)
            if i == pieces - 1:
                mass = own_mass(head)
                for r in received:
                    old = sums[d, source(r) + 1, state_rows:, :].astype(F32)
                    mass = mass + old[:8] + old[8:]
                sums[d, slot, state_rows:, :] = split(mass)
            rs_copy(m, d, i).start()

        def first_way(i):
            return DOWN if i < seqs else UP

        def other_here(m):
            part_copy(head_at(ROLES[m])).wait_recv()
            part_copy(head_at(-ROLES[m])).wait_recv()

        def side(m, some):
            for i in some:
                if i == seqs:
                    other_here(m)
                for d in both:
                    add_and_send(m, d, i)

        own_half, other_half = range(seqs), range(seqs, pieces)

        for i in range(pieces):
            if i == seqs:
                part_copy(head_at(nz // 2)).wait_recv()
            add_and_send(0, first_way(i), i)
        prepare_rest()
        for i in range(pieces):
            if i == seqs:
                other_here(1)
            add_and_send(1, 1 - first_way(i), i)
            add_and_send(1, first_way(i), i, (0,))
        side(SIDE_FAR, own_half)
        for load in late_loads:
            load.wait()
        sides = {2: (SIDE_FAR, other_half), 3: (SIDE_NEAR, own_half), 4: (SIDE_NEAR, other_half)}
        for m in range(2, 6):
            for i in range(pieces):
                if i == seqs:
                    other_here(m)
                for d in both:
                    add_and_send(m, d, i, (m - 1, SIDE_FAR) if m == 5 else (m - 1,))
            if m in sides:
                side(*sides[m])

            @pl.loop((m - 2) * late_units // 4, (m - 1) * late_units // 4)
            def _(unit):
                relayout_late(unit)

        order = list(other_half) + list(own_half)
        part_copy(z).wait_recv()
        for i in order:
            start = i * size
            value = own_sum(z, i)
            for m, d in ((SIDE_NEAR, DOWN), (SIDE_NEAR, UP), (5, DOWN), (5, UP)):
                rs_copy(m, d, i).wait_recv()
                value = value + sums[d, source(m) + 1, start:start + size, :].astype(F32)
            states[z, start:start + size, :] = (value * (1.0 / count)).astype(BF16)
            if i == pieces - 1:
                mass = own_mass(z)
                for m in (SIDE_NEAR, 5):
                    for d in (DOWN, UP):
                        old = sums[d, source(m) + 1, state_rows:, :].astype(F32)
                        mass = mass + old[:8] + old[8:]
                states[z, state_rows:, :] = split(mass * (1.0 / count))
            ag_copy(0, UP, i).start()
            ag_copy(0, DOWN, i).start()
            if i == pieces - 1:
                hand_copy(z).start()

        def hand_pair(distance):
            hand_copy(head_at(-distance)).start()
            hand_copy(head_at(distance)).start()

        def side_copies(m, some):
            for i in some:
                for d in both:
                    ag_copy(m, d, i).start()

        def pass_on(m, work, extra=()):
            for slot, i in enumerate(order):
                if m < 5:
                    for d in both:
                        ag_arrived(m - 1, d, i)
                        ag_copy(m, d, i).start()
                else:
                    for d in (UP, DOWN):
                        ag_arrived(m - 1, d, i)
                    ag_copy(m, 1 - first_way(i), i).start()
                if i == pieces - 1:
                    hand_pair(HELD[m])
                for d in (UP, DOWN):
                    rs_copy(m, d, i).wait_send()
                if slot < pieces - 1:
                    work(slot)
            for side_m, some in extra:
                side_copies(side_m, some)
            work(pieces - 1)

        def side_came(m):
            for i in order:
                for d in both:
                    ag_arrived(m, d, i)
                if i == pieces - 1:
                    hand_pair(HELD[m] + AG_HOPS[m])

        def gone(*messages):
            for m in messages:
                for i in range(pieces):
                    for d in (UP, DOWN):
                        ag_copy(m, d, i).wait_send()

        def weights_here():
            own_load.wait()
            for offset in range(nx * ny):
                piece = lax.rem(chip + offset, nx * ny)
                push_copy(piece, 0).wait_recv()
                if offset > 0:
                    push_copy(piece, 1).wait_recv()

        def read_slice(distance, slot):
            read_part(head_at(-distance) if slot < seqs else head_at(distance), 0, slot % seqs)

        def project_slice(distance, slot, first=False):
            project_part(head_at(-distance), head_at(distance), slot, first)

        def work_1(slot):
            if slot < seqs:
                read_part(z, 0, slot)

        def work_2(slot):
            read_slice(2, slot)

        def work_3(slot):
            read_slice(4, slot)

        def work_4(slot):
            read_slice(5, slot)
            read_slice(1, slot)
            project_slice(2, slot, True)
            project_slice(4, slot)

        def work_5(slot):
            read_slice(6, slot)
            read_slice(3, slot)
            project_slice(5, slot)
            project_slice(1, slot)

        side_copies(SIDE_NEAR, other_half)
        pass_on(1, work_1, ((SIDE_NEAR, own_half),))
        pass_on(2, work_2, ((SIDE_FAR, other_half),))
        pass_on(3, work_3, ((SIDE_FAR, own_half),))
        weights_here()
        side_came(SIDE_NEAR)
        pass_on(4, work_4, ())
        side_came(SIDE_FAR)
        pass_on(5, work_5)
        own_copy().wait_send()
        for slot in range(pieces):
            read_slice(7, slot)
            project_slice(6, slot)
        for slot in range(pieces):
            project_slice(3, slot)
        for i in range(pieces):
            rs_copy(0, first_way(i), i).wait_send()
            for d in (UP, DOWN):
                rs_copy(SIDE_FAR, d, i).wait_send()
                rs_copy(SIDE_NEAR, d, i).wait_send()
        gone(0, 1, 2, SIDE_NEAR)
        end = nz // 2
        for slot, i in enumerate(order):
            ag_arrived(5, 1 - first_way(i), i)
            if i == pieces - 1:
                hand_copy(head_at(end)).start()
            if slot < seqs:
                for part_at in (2 * slot, 2 * slot + 1):
                    project_slice(7, part_at)
            else:
                read_part(head_at(end), 0, slot - seqs)
        project(z, head_at(end), last=True)

        gone(3, 4, SIDE_FAR)
        for i in range(pieces):
            ag_copy(5, 1 - first_way(i), i).wait_send()

        @pl.loop(0, nz)
        def _(j):
            hand_copy(j).wait_send()

    @pl.when(core == 0)
    def _weights():
        start_loads()
        east, west = y * nx + lax.rem(x + 1, nx), y * nx + lax.rem(x + nx - 1, nx)
        north, south = lax.rem(y + 1, ny) * nx + x, lax.rem(y + ny - 1, ny) * nx + x
        ways = ((east, west), (north, south))
        for device in (east, west, north, south):
            pl.semaphore_signal(barrier, inc=1, device_id={"fsdp": device * 2}, device_id_type=MESH)
        pl.semaphore_signal(barrier, inc=1, device_id=partner, device_id_type=MESH)

        items = (((0, 0), (1, 0), (1, -1), (1, 1), (1, 2)), ((1, 0), (0, 0), (0, -1), (0, 1), (0, 2)))

        def piece_at(axis, item, along):
            across = items[axis][item][1]
            dx, dy = (along, across) if axis == 0 else (across, along)
            return lax.rem(y + dy + ny, ny) * nx + lax.rem(x + dx + nx, nx)

        def line_copy(axis, item, way, stage, arriving):
            sign = 1 if way == 0 else -1
            if stage == 0:
                along, start, rows = 0, 0, half
            else:
                along, start, rows = -sign, way * (half // 2), half // 2
            if arriving:
                along = along - sign
                along = 2 if along == -2 else along
            spot = weight.at[piece_at(axis, item, along), pl.ds(items[axis][item][0] * half + start, rows)]
            return pltpu.make_async_remote_copy(
                spot, spot, line_send.at[axis, item, way, stage], line_recv.at[axis, item, way, stage],
                device_id={"fsdp": ways[axis][way] * 2}, device_id_type=MESH,
            )

        def send(axis, item):
            for way in (0, 1):
                line_copy(axis, item, way, 0, False).start()

        def got(axis, item, stage):
            for way in (0, 1):
                line_copy(axis, item, way, stage, True).wait_recv()

        def forward(axis, item):
            for way in (0, 1):
                line_copy(axis, item, way, 0, True).wait_recv()
                line_copy(axis, item, way, 1, False).start()

        def at(dx, dy):
            return lax.rem(y + dy + ny, ny) * nx + lax.rem(x + dx + nx, nx)

        def push(dx, dy, which):
            push_copy(at(dx, dy), which).start()

        prepare_first()
        pl.semaphore_wait(barrier, 5)
        part_copy(head_at(nz // 2)).start()
        prepare_rest()

        part_order = (7, 3, 6, 5, 1, 4, 2)
        for distance in part_order[:2]:
            part_copy(head_at(-distance)).start()
            part_copy(head_at(distance)).start()
        own_load.wait()
        send(0, 0)
        send(1, 1)
        for distance in part_order[2:]:
            part_copy(head_at(-distance)).start()
            part_copy(head_at(distance)).start()
        part_copy(z).start()
        own_copy().wait_recv()
        send(1, 0)
        send(0, 1)
        push(0, 0, 0)
        for load in late_loads:
            load.wait()

        @pl.loop(0, late_units)
        def _(i):
            relayout_late(i)

        forward(0, 0)
        send(1, 2)
        send(1, 3)
        push(-1, 0, 0)
        push(1, 0, 0)
        forward(1, 0)
        send(0, 2)
        send(0, 3)
        push(0, -1, 1)
        push(0, 1, 1)

        forward(0, 1)
        forward(1, 1)
        push(-1, 0, 1)
        push(1, 0, 1)
        push(0, -1, 0)
        push(0, 1, 0)
        got(0, 0, 1)
        send(1, 4)
        push(2, 0, 0)
        got(1, 0, 1)
        send(0, 4)
        push(0, 2, 1)
        for item, off in ((2, -1), (3, 1)):
            forward(1, item)
            push(off, -1, 0)
            push(off, 1, 0)
            forward(0, item)
            push(-1, off, 1)
            push(1, off, 1)
        got(0, 1, 1)
        push(2, 0, 1)
        got(1, 1, 1)
        push(0, 2, 0)
        forward(1, 4)
        push(2, -1, 0)
        push(2, 1, 0)
        forward(0, 4)
        push(-1, 2, 1)
        push(1, 2, 1)
        for item, off in ((2, -1), (3, 1), (4, 2)):
            got(1, item, 1)
            push(off, 2, 0)
            got(0, item, 1)
            push(2, off, 1)

        for axis in (0, 1):
            for item in range(5):
                for way in (0, 1):
                    for stage in (0, 1):
                        line_copy(axis, item, way, stage, False).wait_send()

        @pl.loop(0, nz)
        def _(j):
            part_copy(j).wait_send()

        hand_copy(z).wait_recv()
        read_head(z, seqs)

        def read_pair(k):
            for head in (head_at(-k), head_at(k)):
                hand_copy(head).wait_recv()
                read_head(head, seqs)

        read_pair(2)
        project(head_at(-2), head_at(2), first=True)
        for offset in range(nx * ny):
            piece = lax.rem(chip + offset, nx * ny)
            push_copy(piece, 0).wait_send()
            if offset > 0:
                push_copy(piece, 1).wait_send()

        for k in (4, 5, 1, 6, 3, 7):
            read_pair(k)
            project(head_at(-k), head_at(k))

        hand_copy(head_at(nz // 2)).wait_recv()
        read_head(head_at(nz // 2), seqs)
        project(z, head_at(nz // 2), last=True)


def local(ny, nx, nz, query_rows, key_rows, value_rows, gate_rows, out_weight):
    seqs, tokens, heads, size = query_rows.shape
    rows, width = out_weight.shape
    chips = nx * ny
    raw = pltpu.VMEM((seqs, tokens, heads, size), BF16)
    split = pltpu.VMEM((heads, seqs, tokens, size), BF16)
    part = pltpu.VMEM((heads, seqs * size + 8, size), F32)
    chunk = 2 * seqs * size + 16
    dma = pltpu.SemaphoreType.DMA
    return pl.pallas_call(
        functools.partial(layer_kernel, ny, nx, nz, float(tokens * nz)),
        name="layer",
        out_shape=jax.ShapeDtypeStruct((seqs, tokens, width), BF16),
        in_specs=[pl.BlockSpec(memory_space=pltpu.HBM)] * 5,
        out_specs=pl.BlockSpec(memory_space=pltpu.VMEM),
        scratch_shapes=[
            raw, raw, raw, raw,
            split, split, split,
            pltpu.VMEM((heads, seqs, tokens, size), F32),
            part, part,
            pltpu.VMEM((2, 11, chunk, size), BF16),
            pltpu.VMEM((heads, chunk, size), BF16),
            pltpu.VMEM((chips, 2 * rows, width), BF16),
            pltpu.VMEM((heads, seqs * tokens, size), BF16),
            pltpu.VMEM((seqs * tokens, width), F32),
            dma((4, seqs)),
            dma((heads,)), dma((heads,)),
            dma((8, 2, 2 * seqs)), dma((8, 2, 2 * seqs)),
            dma((8, 2, 2 * seqs)), dma((8, 2, 2 * seqs)),
            dma((heads,)), dma((heads,)),
            dma((2, 5, 2, 2)), dma((2, 5, 2, 2)),
            dma((chips, 2)), dma((chips, 2)),
            dma, dma,
        ],
        compiler_params=pltpu.CompilerParams(
            collective_id=0, has_side_effects=True, vmem_limit_bytes=52 * 2**20
        ),
    )(query_rows, key_rows, value_rows, gate_rows, pltpu.with_memory_space_constraint(out_weight, pltpu.HBM))


def solution(mesh):
    in_specs = (
        P("fsdp", "seq", None, None),
        P("fsdp", "seq", None, None),
        P("fsdp", "seq", None, None),
        P("fsdp", "seq", None, None),
        P("fsdp", None),
    )
    out_specs = P("fsdp", "seq", None)
    body = functools.partial(local, 4, 4, mesh.shape["seq"])
    return jax.shard_map(body, mesh=mesh, in_specs=in_specs, out_specs=out_specs, check_vma=False)
```
